32 devices in a mesh: inter: 2 (over y), intra: 16 (over z, x, core).
Axes of the slice: x: 2, y: 2, z: 4, core: 2. Of those that a mesh axis runs over, the one named last changes fastest.
Arguments:
- activations: bfloat16 [65536, 4096], P(('inter', 'intra')), may hold values from -6 to 6
- key_cotangent: bfloat16 [65536, 512], P(('inter', 'intra')), may hold values from -0.046875 to 0.046875
- value_cotangent: bfloat16 [65536, 512], P(('inter', 'intra')), may hold values from -0.046875 to 0.046875
Outputs:
- grad_key: float32 [4096, 512], P('intra')
- grad_value: float32 [4096, 512], P('intra')
The draws below stay inside these ranges and needn't reach their ends.
All inputs are finite; a program needn't handle non-finite values.
Results may differ from the reference program's by a relative error of at most 0.0029.
Values sent between devices are 32-bit elements; how exact they have to be, the bound alone decides.
A program may use at most 128 MiB of HBM per device.

```python
import jax
import jax.numpy as jnp
from jax import lax

D = 4096
TOK_DEV = 2048
KV = 512
TOKENS = 65536
N_INTER = 2
N_INTRA = 16


def levels(key, dims, split, low, largest):
    level, own = 1.0, jax.random.fold_in(key, 6)
    for dim, blocks in split:
        heights = jnp.exp(jax.random.uniform(jax.random.fold_in(own, dim), (blocks,), jnp.float32, low / len(split), largest / len(split)))
        level = level * jnp.repeat(heights, dims[dim] // blocks).reshape([-1 if axis == dim else 1 for axis in range(len(dims))])
    return level


def centred(stream_key, shape, spread, limit, cuts=(), kind=jnp.bfloat16):
    values = spread * jax.random.normal(stream_key, shape, jnp.float32)
    if cuts:
        values = values * levels(stream_key, shape, cuts, -0.22, 0.18)
    return jnp.clip(values, -limit, limit).astype(kind)


def setup_inputs(seed: int = 0) -> dict:
    arg_keys = jax.random.split(jax.random.key(seed), 4)
    activations = centred(arg_keys[0], (TOKENS, D), 1.0, 6.0, ((0, 32),))
    key_cotangent = centred(arg_keys[1], (TOKENS, KV), 0.003, 0.046875, ((0, 32),))
    value_cotangent = centred(arg_keys[2], (TOKENS, KV), 0.003, 0.046875, ((0, 32),))
    return dict(activations=activations, key_cotangent=key_cotangent, value_cotangent=value_cotangent)


def accumulate(total, inputs):
    rows, cotangent = inputs
    device_term = jnp.dot(rows.T, cotangent, preferred_element_type=jnp.float32)
    rounded = lax.optimization_barrier(device_term.astype(jnp.bfloat16))
    return total + rounded.astype(jnp.float32), None


def reference(activations, key_cotangent, value_cotangent):
    devices = N_INTER * N_INTRA
    stacked_rows = activations.reshape(devices, TOK_DEV, D)
    cotangent = jnp.concatenate((key_cotangent, value_cotangent), axis=1).reshape(devices, TOK_DEV, 2 * KV)
    total = lax.scan(accumulate, jnp.zeros((D, 2 * KV), jnp.float32), (stacked_rows, cotangent))[0]
    return total[:, :KV], total[:, KV:]
```

```python
import functools
import heapq

import jax
import jax.numpy as jnp
from jax import lax
from jax.experimental import pallas as pl
from jax.experimental.pallas import tpu as pltpu
from jax.sharding import PartitionSpec as P

MESH = pl.DeviceIdType.MESH
PARTS = (
    ('xzy', 0, 4, 0),
    ('xzy', 0, 3, 2),
    ('yxz', 0, 4, 1),
    ('yxz', 0, 3, 3),
    ('zxy', 3, 1, 2),
    ('zxy', 3, 1, 3),
)
TUNE = {
    "first": 5.0, "step": 1.55, "latency": 1.9, "ahead": 4.0,
    "rate": 46.6e3, "margin": 1.0, "cost": 0.08, "rank": {},
}


class Message:
    def __init__(self, part, stage, kind, sender, block, receiver, target, rows, split, slot):
        self.part, self.stage, self.kind = part, stage, kind
        self.sender, self.block = sender, block
        self.receiver, self.target = receiver, target
        self.rows, self.split, self.slot = rows, split, slot


def plan_messages(groups, parts):
    roles, messages = groups // 2, []
    for part, (order, _, rows, _, _) in enumerate(parts):
        split, reduced, sides = False, False, (0, 1)

        def add(stage, kind, sender, block, receiver, target, name):
            slot = (part, stage, name)
            messages.append(
                Message(part, stage, kind, sender, block, receiver, target, rows, split, slot)
            )

        for stage, axis in enumerate(order):
            last = stage == len(order) - 1
            if axis == "x":
                sides = (0,)
            elif axis == "y" and not last:
                rows, split = rows // 2, True
            for role in range(roles):
                own = [role] if reduced else range(groups)
                if axis == "x":
                    for q in own:
                        name = ("x", -1 if reduced else q)
                        add(stage, "x", role, (q, 1), role, (q, 0), name)
                elif axis == "y" and last:
                    add(stage, "both", role, (role, 0), role, (role, 0), ("both",))
                elif axis == "y":
                    for q in own:
                        for side in sides:
                            name = ("y", -1 if reduced else q, side)
                            add(stage, "y", role, (q, side), role, (q, side), name)
                else:
                    for side in sides:
                        for q in range(role + 1, groups):
                            if role + 1 < roles:
                                name, there, to = ("in", q, side), q, role + 1
                            else:
                                there, to = groups - 1 - q, role
                                name = ("across", there, side)
                            add(stage, "in", role, (q, side), to, (there, side), name)
                        for q in range(role):
                            name = ("out", q, side)
                            add(stage, "out", role, (q, side), role - 1, (q, side), name)
            reduced = reduced or axis == "z"
        if split:
            for role in range(roles):
                add(len(order), "gather", role, (role, 0), role, (role, 0), ("gather",))
    return messages


def link_of(message):
    kind = message.kind
    return message.sender, "y" if kind in ("both", "gather") else kind


def schedule(groups, parts, messages, order, half, rows):
    tune = TUNE
    roles = groups // 2
    ready_at = {(k, h): tune["first"] + tune["step"] * (2 * i + h) for i, k in enumerate(order) for h in (0, 1)}
    latency, ahead = tune["latency"], tune["ahead"]
    steps = sorted(ready_at.values())
    incoming, leaving = {}, {}
    for message in messages:
        incoming.setdefault((message.receiver, message.part, message.target), []).append(message)
        leaving.setdefault((message.sender, message.part, message.block), []).append(message)

    def needed(message):
        before = incoming.get((message.sender, message.part, message.block), [])
        toward = message.kind in ("in", "out")
        return [
            o for o in before
            if o.stage < message.stage
            or (toward and o.stage == message.stage and not (message.kind == "out" and o.slot[2][0] == "in")
                and not (message.kind == "in" and o.slot[2][0] in ("out", "across")))
        ]

    need = {m: needed(m) for m in messages}
    feeds = {m: [] for m in messages}
    for m in messages:
        for o in need[m]:
            feeds[o].append(m)

    def length(message):
        return message.rows * parts[message.part][4] * 4 / tune["rate"]

    @functools.cache
    def tail(message):
        return latency + length(message) + max((tail(o) for o in feeds[message]), default=0.0)

    def priority(message):
        return tail(message) + tune["rank"].get((message.part, message.stage), 0.0)

    def depth(message):
        return 0 if parts[message.part][3] < half else 1

    slots = {(role, i, h): [] for role in range(roles) for i in range(len(order)) for h in (0, 1)}
    final = {role: [] for role in range(roles)}
    left = {m: len(need[m]) for m in messages}
    computed, queued = set(), {}
    free, arrivals, serial = {}, [], 0
    names = {value: (i, h) for i, k in enumerate(order) for h in (0, 1) for value in [ready_at[k, h]]}
    events = [(at, 0, role, "step", at) for at in steps for role in range(roles)]
    heapq.heapify(events)
    number = len(events)
    waiting = {role: [] for role in range(roles)}
    pending = {role: len(steps) for role in range(roles)}
    clock = {role: 0.0 for role in range(roles)}
    end = 0.0
    busy = {}

    def enqueue(message):
        queued.setdefault(link_of(message), []).append(message)

    def release(role, now):
        nonlocal number
        started = []
        for link, queue in queued.items():
            if link[0] != role or not queue:
                continue
            queue.sort(key=priority, reverse=True)
            while queue and (free.get(link, 0.0) - now < ahead or not pending[role]):
                message = queue.pop(0)
                begin = max(now, free.get(link, 0.0))
                free[link] = begin + length(message)
                busy.setdefault(link, []).append((begin, free[link], message))
                number += 1
                pending[message.receiver] += 1
                heapq.heappush(events, (free[link] + latency, number, message.receiver, "arrival", message))
                started.append(message)
        return started

    def accept(message):
        pending[message.receiver] -= 1
        for later in feeds[message]:
            left[later] -= 1
            if not left[later] and (later.block, depth(later)) in computed_of[later.sender]:
                enqueue(later)

    computed_of = {role: set() for role in range(roles)}
    last = steps[-1]
    while events:
        now, _, role, what, item = heapq.heappop(events)
        if what == "arrival" and now < last:
            waiting[role].append((now, item))
            continue
        if what == "step":
            pending[role] -= 1
            i, h = names[item]
            k = order[i]
            computed_of[role].add((k, h))
            for message in messages:
                if message.sender == role and message.block == k and depth(message) == h and not left[message]:
                    enqueue(message)
            slots[role, i, h].append((None, release(role, now)))
            for entry in list(waiting[role]):
                arrived, message = entry
                if (arrived < now - tune["margin"] or now == last) and (message.target, depth(message)) in computed_of[role]:
                    waiting[role].remove(entry)
                    accept(message)
                    target = final[role] if now == last else slots[role, i, h]
                    target.append((message, release(role, now)))
            if now == last:
                final[role].insert(0, (None, []))
            continue
        now = max(now, clock[role])
        clock[role] = now + tune["cost"]
        accept(item)
        final[role].append((item, release(role, now)))
        end = max(end, clock[role])
    assert not any(queued.values()) and not any(waiting.values())
    return slots, final


def block_order(groups):
    return [(q, side) for q in reversed(range(groups)) for side in (1, 0)]


def kernel(
    mesh_shape, parts, messages, order, plan,
    a_hbm, key_hbm, value_hbm, key_out, value_out,
    a_ref, cot_ref, pair_ref, mate_ref, *rest,
):
    shapes = landing_shapes(parts, messages)
    landing = dict(zip(shapes, rest))
    a_sem, cot_sem, mate_send, mate_recv, send_sem, recv_sem = rest[len(shapes):]
    slots, final = plan
    groups = mesh_shape["intra"] // 4
    roles = groups // 2
    blocks = 2 * groups
    rows = key_out.shape[0]
    tall = 2 * rows
    half = key_hbm.shape[1]
    place = {k: i for i, k in enumerate(order)}
    numbers = {name: i for i, name in enumerate(sorted({m.slot for m in messages}, key=str))}
    indices = landing_indices(parts, messages)

    y = lax.axis_index("inter")
    me = lax.axis_index("intra")
    core = me % 2
    x = (me // 2) % 2
    group = me // 4
    far = group // roles
    role = group + far * (groups - 1 - 2 * group)
    inward = 4 * (1 - 2 * far)

    def partner(kind):
        if kind == "core":
            return {"intra": me + 1 - 2 * core}
        if kind == "x":
            return {"intra": me + 2 * (1 - 2 * x)}
        if kind == "in":
            return {"intra": me + inward}
        if kind == "out":
            return {"intra": me - inward}
        return {"inter": 1 - y}

    cot_copies = [
        pltpu.make_async_copy(key_hbm, cot_ref.at[:, pl.ds(0, half)], cot_sem.at[0]),
        pltpu.make_async_copy(value_hbm, cot_ref.at[:, pl.ds(half, half)], cot_sem.at[1]),
    ]
    cot_copies[0].start()

    def a_copy(i, k):
        q, side = k
        block = 2 * (q + far * (groups - 1 - 2 * q)) + (x + side) % 2
        columns = pl.ds(pl.multiple_of(block * tall, tall), tall)
        return pltpu.make_async_copy(a_hbm.at[:, columns], a_ref.at[i], a_sem.at[i])

    a_copy(0, order[0]).start()

    barrier = pltpu.get_barrier_semaphore()
    neighbours = ["core", "x", "y", "in"]
    for kind in neighbours:
        pl.semaphore_signal(barrier, inc=1, device_id=partner(kind), device_id_type=MESH)

    @pl.when(role > 0)
    def _():
        pl.semaphore_signal(barrier, inc=1, device_id=partner("out"), device_id_type=MESH)

    @pl.when(role > 0)
    def _():
        pl.semaphore_wait(barrier, len(neighbours) + 1)

    @pl.when(role == 0)
    def _():
        pl.semaphore_wait(barrier, len(neighbours))

    def side_of(h):
        return pl.ds(h * half, half)

    def mate_copy(i, h):
        return pltpu.make_async_remote_copy(
            src_ref=pair_ref.at[i, 1 - core, :, side_of(h)],
            dst_ref=mate_ref.at[i, h],
            send_sem=mate_send.at[i, h],
            recv_sem=mate_recv.at[i, h],
            device_id=partner("core"),
            device_id_type=MESH,
        )

    def rows_of(message, mine):
        base = parts[message.part][1]
        if not message.split:
            return pl.ds(base, message.rows)
        half_of = y if mine else 1 - y
        return pl.ds(pl.multiple_of(base + half_of * message.rows, 8), message.rows)

    def columns_of(message):
        return pl.ds(parts[message.part][3], parts[message.part][4])

    def result(message, mine):
        base, width = parts[message.part][3:]
        out, start = (key_out, base) if base < half else (value_out, base - half)
        return out.at[rows_of(message, mine), pl.ds(start, width)]

    def kept(message, block):
        return pair_ref.at[place[block], core, rows_of(message, True), columns_of(message)]

    def arrived(message):
        shape = message.rows, parts[message.part][4]
        return landing[shape].at[indices[message.slot]]

    def remote(message):
        number = numbers[message.slot]
        mine = message.kind != "y"
        return pltpu.make_async_remote_copy(
            src_ref=pair_ref.at[
                place[message.block], core, rows_of(message, mine), columns_of(message)
            ],
            dst_ref=arrived(message),
            send_sem=send_sem.at[number],
            recv_sem=recv_sem.at[number],
            device_id=partner(message.kind),
            device_id_type=MESH,
        )

    def perform(actions):
        for message, follow in actions:
            if message is not None:
                remote(message).wait_recv()
                if message.kind == "both":
                    total = kept(message, message.target)[...] + arrived(message)[...]
                    result(message, True)[...] = total
                elif message.kind == "gather":
                    result(message, False)[...] = arrived(message)[...]
                else:
                    kept(message, message.target)[...] += arrived(message)[...]
            for later in follow:
                remote(later).start()
                if later.kind == "gather":
                    result(later, True)[...] = kept(later, later.block)[...]

    def finish(i, h):
        mate_copy(i, h).wait_recv()
        pair_ref[i, core, :, side_of(h)] += mate_ref[i, h]
        for r in range(roles):
            for j in range(blocks):
                if any(message or follow for message, follow in slots[r, j, h]):
                    @pl.when((i == j) & (role == r))
                    def _():
                        perform(slots[r, j, h])

    def multiply(i, h):
        product = lax.dot_general(
            a_ref[i], cot_ref[:, side_of(h)], (((0,), (0,)), ((), ())),
            preferred_element_type=jnp.float32,
        )
        rounded = product.astype(jnp.bfloat16).astype(jnp.float32)
        pair_ref[i, :, :, side_of(h)] = rounded.reshape(2, rows, half)
        mate_copy(i, h).start()

    cot_copies[0].wait()

    def body(i, carry):
        pltpu.make_async_copy(
            a_hbm.at[:, pl.ds(0, tall)], a_ref.at[i], a_sem.at[i]
        ).wait()

        @pl.when(i == 0)
        def _():
            cot_copies[1].start()

        for j, k in enumerate(order[1:]):
            @pl.when(i == j)
            def _():
                a_copy(j + 1, k).start()

        multiply(i, 0)

        @pl.when(i > 0)
        def _():
            finish(i - 1, 1)

        @pl.when(i == 0)
        def _():
            cot_copies[1].wait()

        multiply(i, 1)
        finish(i, 0)
        return carry

    lax.fori_loop(0, blocks, body, 0)
    finish(blocks - 1, 1)

    for r in range(roles):
        @pl.when(role == r)
        def _():
            perform(final[r])
            for message in messages:
                if message.sender == r:
                    remote(message).wait_send()

    for i in range(blocks):
        for h in range(2):
            mate_copy(i, h).wait_send()


def landing_indices(parts, messages):
    counts, indices = {}, {}
    for message in messages:
        shape = message.rows, parts[message.part][4]
        if message.slot not in indices:
            indices[message.slot] = counts.get(shape, 0)
            counts[shape] = counts.get(shape, 0) + 1
    return indices


def landing_shapes(parts, messages):
    counts = {}
    for slot, message in {m.slot: m for m in messages}.items():
        shape = message.rows, parts[message.part][4]
        counts[shape] = counts.get(shape, 0) + 1
    return dict(sorted(counts.items(), reverse=True))


def cut(rows, columns):
    return tuple(
        (way, rows * top // 4, rows * tall // 4, columns * left // 4, columns // 4)
        for way, top, tall, left in PARTS
    )


def local(mesh_shape, activations, key_cotangent, value_cotangent):
    tokens, width = activations.shape
    half = key_cotangent.shape[1]
    rows = width // mesh_shape["intra"]
    groups = mesh_shape["intra"] // 4
    blocks = 2 * groups
    parts = cut(rows, 2 * half)
    messages = plan_messages(groups, parts)
    order = block_order(groups)
    plan = schedule(groups, parts, messages, order, half, rows)
    names = {message.slot for message in messages}
    f32 = jnp.float32
    landing = [
        pltpu.VMEM((count, *shape), f32)
        for shape, count in landing_shapes(parts, messages).items()
    ]
    totals = pl.pallas_call(
        functools.partial(kernel, mesh_shape, parts, messages, order, plan),
        out_shape=(pltpu.VMEM((rows, half), f32),) * 2,
        in_specs=[pl.BlockSpec(memory_space=pl.ANY)] * 3,
        out_specs=(pl.BlockSpec(memory_space=pltpu.VMEM),) * 2,
        scratch_shapes=[
            pltpu.VMEM((blocks, tokens, 2 * rows), activations.dtype),
            pltpu.VMEM((tokens, 2 * half), key_cotangent.dtype),
            pltpu.VMEM((blocks, 2, rows, 2 * half), f32),
            pltpu.VMEM((blocks, 2, rows, half), f32),
            *landing,
            pltpu.SemaphoreType.DMA((blocks,)),
            pltpu.SemaphoreType.DMA((2,)),
            pltpu.SemaphoreType.DMA((blocks, 2)),
            pltpu.SemaphoreType.DMA((blocks, 2)),
            pltpu.SemaphoreType.DMA((len(names),)),
            pltpu.SemaphoreType.DMA((len(names),)),
        ],
        compiler_params=pltpu.CompilerParams(
            collective_id=0, has_side_effects=True, vmem_limit_bytes=65900000
        ),
    )(activations, key_cotangent, value_cotangent)
    shape = jax.ShapeDtypeStruct((rows, half), f32)
    return pl.pallas_call(
        write_out,
        out_shape=(shape, shape),
        in_specs=[pl.BlockSpec(memory_space=pltpu.VMEM)] * 2,
        out_specs=(pl.BlockSpec(memory_space=pltpu.HBM),) * 2,
        scratch_shapes=[pltpu.SemaphoreType.DMA((2,))],
    )(*[pltpu.with_memory_space_constraint(total, pltpu.VMEM) for total in totals])


def write_out(key_ref, value_ref, key_out, value_out, sem):
    copies = [
        pltpu.make_async_copy(key_ref, key_out, sem.at[0]),
        pltpu.make_async_copy(value_ref, value_out, sem.at[1]),
    ]
    for copy in copies:
        copy.start()
    for copy in copies:
        copy.wait()


def solution(mesh):
    mesh_shape = dict(mesh.shape)
    return jax.shard_map(
        functools.partial(local, mesh_shape),
        mesh=mesh,
        in_specs=(
            P(("inter", "intra"), None),
            P(("inter", "intra"), None),
            P(("inter", "intra"), None),
        ),
        out_specs=(P("intra", None), P("intra", None)),
        check_vma=False,
    )
```

```python
import functools
import heapq

import jax
import jax.numpy as jnp
from jax import lax
from jax.experimental import pallas as pl
from jax.experimental.pallas import tpu as pltpu
from jax.sharding import PartitionSpec as P

MESH = pl.DeviceIdType.MESH
PARTS = (
    ('zxy', 0, 2, 0, 2),
    ('xzy', 2, 6, 0, 2),
    ('yxz', 0, 8, 2, 1),
    ('yxz', 0, 8, 3, 1),
    ('xyz', 0, 8, 4, 2),
    ('zyx', 0, 4, 6, 2),
    ('yxz', 4, 4, 6, 2),
)
TUNE = {
    "first": 4.75, "strip": 2.0, "second": 8.75, "step": 1.6, "latency": 1.95, "ahead": 4.0, "rate": 46600.0, "margin": 1.0, "cost": 0.08,
    "rank": {(4, 2): 121.1, (5, 2): 155.2, (7, 1): -70.5, (3, 3): -52.4, (5, 3): 15.9, (5, 0): -73.3, (0, 2): 28.0, (2, 2): -88.9, (2, 1): -13.3, (3, 1): -10.6, (4, 0): 77.0, (2, 0): -106.9, (0, 0): 117.3, (1, 0): 7.7, (3, 0): 9.8, (7, 2): -54.5, (6, 3): 73.9, (0, 1): 98.3, (7, 3): -53.2, (6, 1): -12.3, (1, 2): 76.7, (1, 3): 151.0, (4, 1): -83.1, (0, 3): -77.9, (7, 0): 49.0, (6, 2): 134.3, (3, 2): -71.0, (5, 1): 115.5, (1, 1): -34.7, (4, 3): -9.1, (2, 3): -114.1, (6, 0): 20.8, (8, 0): -53.1, (9, 1): -30.5, (9, 2): 35.7, (9, 3): -16.7, (8, 2): -3.5, (8, 1): 109.4, (9, 0): 12.0, (8, 3): -52.0},
}


class Message:
    def __init__(self, part, stage, kind, sender, block, receiver, target, rows, split, slot):
        self.part, self.stage, self.kind = part, stage, kind
        self.sender, self.block = sender, block
        self.receiver, self.target = receiver, target
        self.rows, self.split, self.slot = rows, split, slot


def plan_messages(groups, parts):
    roles, messages = groups // 2, []
    for part, (order, _, rows, _, _) in enumerate(parts):
        split, reduced, sides = False, False, (0, 1)

        def add(stage, kind, sender, block, receiver, target, name):
            slot = (part, stage, name)
            messages.append(
                Message(part, stage, kind, sender, block, receiver, target, rows, split, slot)
            )

        for stage, axis in enumerate(order):
            last = stage == len(order) - 1
            if axis == "x":
                sides = (0,)
            elif axis == "y" and not last:
                rows, split = rows // 2, True
            for role in range(roles):
                own = [role] if reduced else range(groups)
                if axis == "x":
                    for q in own:
                        name = ("x", -1 if reduced else q)
                        add(stage, "x", role, (q, 1), role, (q, 0), name)
                elif axis == "y" and last:
                    add(stage, "both", role, (role, 0), role, (role, 0), ("both",))
                elif axis == "y":
                    for q in own:
                        for side in sides:
                            name = ("y", -1 if reduced else q, side)
                            add(stage, "y", role, (q, side), role, (q, side), name)
                else:
                    for side in sides:
                        for q in range(role + 1, groups):
                            if role + 1 < roles:
                                name, there, to = ("in", q, side), q, role + 1
                            else:
                                there, to = groups - 1 - q, role
                                name = ("across", there, side)
                            add(stage, "in", role, (q, side), to, (there, side), name)
                        for q in range(role):
                            name = ("out", q, side)
                            add(stage, "out", role, (q, side), role - 1, (q, side), name)
            reduced = reduced or axis == "z"
        if split:
            for role in range(roles):
                add(len(order), "gather", role, (role, 0), role, (role, 0), ("gather",))
    return messages


def link_of(message):
    kind = message.kind
    return message.sender, "y" if kind in ("both", "gather") else kind


def compute_steps(order, half, tune):
    steps = []
    for i, k in enumerate(order):
        for h in (0, 1):
            at = tune["second"] + tune["step"] * (2 * (i - 1) + h)
            if not i:
                at = tune["first"] + tune["strip"] * h
            steps.append((k, h * half, (h + 1) * half, at))
    return steps


def schedule(groups, parts, messages, steps, tune):
    roles, latency = groups // 2, tune["latency"]
    incoming = {}
    for message in messages:
        incoming.setdefault((message.receiver, message.part, message.target), []).append(message)

    def needed(message):
        before = incoming.get((message.sender, message.part, message.block), [])
        same = {"in": ("in",), "out": ("out", "across")}.get(message.kind, ())
        return [
            o for o in before
            if o.stage < message.stage or (o.stage == message.stage and o.slot[2][0] in same)
        ]

    need = {m: needed(m) for m in messages}
    feeds = {m: [] for m in messages}
    for m in messages:
        for o in need[m]:
            feeds[o].append(m)

    def length(message):
        return message.rows * parts[message.part][4] * 4 / tune["rate"]

    @functools.cache
    def tail(message):
        return latency + length(message) + max((tail(o) for o in feeds[message]), default=0.0)

    def priority(message):
        return tail(message) + tune["rank"].get((message.part, message.stage), 0.0)

    def step_of(part, block):
        start = parts[part][3]
        return next(n for n, (k, low, high, _) in enumerate(steps) if k == block and low <= start < high)

    made_in = {m: step_of(m.part, m.block) for m in messages}
    kept_in = {m: step_of(m.part, m.target) for m in messages}
    slots = {(role, n): [] for role in range(roles) for n in range(len(steps))}
    final = {role: [] for role in range(roles)}
    left = {m: len(need[m]) for m in messages}
    done = {role: -1 for role in range(roles)}
    clock = {role: 0.0 for role in range(roles)}
    pending = {role: len(steps) for role in range(roles)}
    waiting = {role: [] for role in range(roles)}
    queued, free = {}, {}
    events = [(step[3], n, role, n, None) for n, step in enumerate(steps) for role in range(roles)]
    heapq.heapify(events)
    number, last = len(events), len(steps) - 1

    def enqueue(message):
        queued.setdefault(link_of(message), []).append(message)

    def release(role, now):
        nonlocal number
        started = []
        for link, queue in queued.items():
            if link[0] != role or not queue:
                continue
            queue.sort(key=priority, reverse=True)
            while queue and (free.get(link, 0.0) - now < tune["ahead"] or not pending[role]):
                message = queue.pop(0)
                begin = max(now, free.get(link, 0.0))
                free[link] = begin + length(message)
                number += 1
                pending[message.receiver] += 1
                heapq.heappush(events, (free[link] + latency, number, message.receiver, None, message))
                started.append(message)
        return started

    def accept(message):
        pending[message.receiver] -= 1
        for later in feeds[message]:
            left[later] -= 1
            if not left[later] and made_in[later] <= done[later.sender]:
                enqueue(later)

    while events:
        now, _, role, n, message = heapq.heappop(events)
        if message is not None:
            if done[role] < last:
                waiting[role].append((now, message))
                continue
            now = max(now, clock[role])
            clock[role] = now + tune["cost"]
            accept(message)
            final[role].append((message, release(role, now)))
            continue
        done[role] = n
        pending[role] -= 1
        for message in messages:
            if message.sender == role and made_in[message] == n and not left[message]:
                enqueue(message)
        slots[role, n].append((None, release(role, now)))
        actions = final[role] if n == last else slots[role, n]
        for entry in list(waiting[role]):
            at, message = entry
            if (at < now - tune["margin"] or n == last) and kept_in[message] <= n:
                waiting[role].remove(entry)
                accept(message)
                actions.append((message, release(role, now)))
    assert not any(queued.values()) and not any(waiting.values())
    return slots, final


def block_order(groups):
    order = [(q, side) for q in reversed(range(groups)) for side in (1, 0)]
    if groups == 4:
        order = [(3, 1), (3, 0), (2, 1), (1, 0), (1, 1), (0, 0), (2, 0), (0, 1)]
    return order


def kernel(
    mesh_shape, parts, messages, order, plan,
    a_hbm, key_hbm, value_hbm, key_out, value_out,
    a_ref, cot_ref, pair_ref, mate_ref, *rest,
):
    shapes = landing_shapes(parts, messages)
    landing = dict(zip(shapes, rest))
    a_sem, first_sem, cot_sem, mate_send, mate_recv, send_sem, recv_sem = rest[len(shapes):]
    slots, final = plan
    groups = mesh_shape["intra"] // 4
    roles = groups // 2
    blocks = 2 * groups
    rows = key_out.shape[0]
    tall = 2 * rows
    half = key_hbm.shape[1]
    place = {k: i for i, k in enumerate(order)}
    numbers = {name: i for i, name in enumerate(sorted({m.slot for m in messages}, key=str))}
    indices = landing_indices(parts, messages)

    y = lax.axis_index("inter")
    me = lax.axis_index("intra")
    core = me % 2
    x = (me // 2) % 2
    group = me // 4
    far = group // roles
    role = group + far * (groups - 1 - 2 * group)
    inward = 4 * (1 - 2 * far)

    def partner(kind):
        if kind == "core":
            return {"intra": me + 1 - 2 * core}
        if kind == "x":
            return {"intra": me + 2 * (1 - 2 * x)}
        if kind == "in":
            return {"intra": me + inward}
        if kind == "out":
            return {"intra": me - inward}
        return {"inter": 1 - y}

    cot_copies = [
        pltpu.make_async_copy(key_hbm, cot_ref.at[:, pl.ds(0, half)], cot_sem.at[0]),
        pltpu.make_async_copy(value_hbm, cot_ref.at[:, pl.ds(half, half)], cot_sem.at[1]),
    ]

    def a_copy(i, k):
        q, side = k
        block = 2 * (q + far * (groups - 1 - 2 * q)) + (x + side) % 2
        columns = pl.ds(pl.multiple_of(block * tall, tall), tall)
        return pltpu.make_async_copy(a_hbm.at[:, columns], a_ref.at[i], a_sem.at[i])

    def first_copy(owner):
        q, side = order[0]
        block = 2 * (q + far * (groups - 1 - 2 * q)) + (x + side) % 2
        columns = pl.ds(pl.multiple_of((2 * block + owner) * rows, rows), rows)
        lanes = pl.ds(pl.multiple_of(owner * rows, rows), rows)
        index = (owner + core) % 2
        return pltpu.make_async_copy(
            a_hbm.at[:, columns], a_ref.at[0, :, lanes], first_sem.at[index]
        )

    split_first = rows % 128 == 0
    cot_copies[0].start()
    if split_first:
        first_copy(1 - core).start()
    else:
        a_copy(0, order[0]).start()

    barrier = pltpu.get_barrier_semaphore()
    neighbours = ["core", "x", "y", "in"]
    for kind in neighbours:
        pl.semaphore_signal(barrier, inc=1, device_id=partner(kind), device_id_type=MESH)

    @pl.when(role > 0)
    def _():
        pl.semaphore_signal(barrier, inc=1, device_id=partner("out"), device_id_type=MESH)

    def side_of(h):
        return pl.ds(h * half, half)

    def mate_copy(i, h):
        return pltpu.make_async_remote_copy(
            src_ref=pair_ref.at[i, 1 - core, :, side_of(h)],
            dst_ref=mate_ref.at[i, h],
            send_sem=mate_send,
            recv_sem=mate_recv.at[i, h],
            device_id=partner("core"),
            device_id_type=MESH,
        )

    def rows_of(message, mine):
        base = parts[message.part][1]
        if not message.split:
            return pl.ds(base, message.rows)
        half_of = y if mine else 1 - y
        return pl.ds(pl.multiple_of(base + half_of * message.rows, 8), message.rows)

    def columns_of(message):
        return pl.ds(parts[message.part][3], parts[message.part][4])

    def result(message, mine):
        base, width = parts[message.part][3:]
        out, start = (key_out, base) if base < half else (value_out, base - half)
        return out.at[rows_of(message, mine), pl.ds(start, width)]

    def kept(message, block):
        return pair_ref.at[place[block], core, rows_of(message, True), columns_of(message)]

    def arrived(message):
        shape = message.rows, parts[message.part][4]
        return landing[shape].at[indices[message.slot]]

    def remote(message):
        number = numbers[message.slot]
        mine = message.kind != "y"
        return pltpu.make_async_remote_copy(
            src_ref=pair_ref.at[
                place[message.block], core, rows_of(message, mine), columns_of(message)
            ],
            dst_ref=arrived(message),
            send_sem=send_sem.at[list(shapes).index((message.rows, parts[message.part][4]))],
            recv_sem=recv_sem.at[number],
            device_id=partner(message.kind),
            device_id_type=MESH,
        )

    def perform(actions):
        for message, follow in actions:
            if message is not None:
                remote(message).wait_recv()
                if message.kind == "both":
                    total = kept(message, message.target)[...] + arrived(message)[...]
                    result(message, True)[...] = total
                elif message.kind == "gather":
                    result(message, False)[...] = arrived(message)[...]
                else:
                    kept(message, message.target)[...] += arrived(message)[...]
            for later in follow:
                remote(later).start()
                if later.kind == "gather":
                    result(later, True)[...] = kept(later, later.block)[...]

    def run(role_steps):
        for r in range(roles):
            for chosen, n in role_steps:
                if any(message or follow for message, follow in slots[r, n]):
                    @pl.when(chosen & (role == r))
                    def _():
                        perform(slots[r, n])

    def product(i, h, lanes):
        exact = lax.dot_general(
            a_ref[i, :, lanes], cot_ref[:, side_of(h)], (((0,), (0,)), ((), ())),
            preferred_element_type=jnp.float32,
        )
        return exact.astype(jnp.bfloat16).astype(jnp.float32)

    def multiply_one(i, h, owner):
        lanes = pl.ds(pl.multiple_of(owner * rows, rows), rows)
        pair_ref[i, owner, :, side_of(h)] = product(i, h, lanes)

    def multiply(i, h, enter=None, between=None):
        whole = not (split_first and isinstance(i, int))
        if whole:
            pair_ref[i, :, :, side_of(h)] = product(i, h, pl.ds(0, tall)).reshape(2, rows, half)
        else:
            multiply_one(i, h, 1 - core)
        if enter:
            enter()
        mate_copy(i, h).start()
        if between and not whole:
            between()
        if not whole:
            multiply_one(i, h, core)

    def finish(i, h):
        mate_copy(i, h).wait_recv()
        pair_ref[i, core, :, side_of(h)] += mate_ref[i, h]
        if isinstance(i, int):
            run([(role >= 0, 2 * i + h)])
        else:
            run([(i == j, 2 * j + h) for j in range(1 - h, blocks - h)])

    def meet():
        @pl.when(role > 0)
        def _():
            pl.semaphore_wait(barrier, len(neighbours) + 1)

        @pl.when(role == 0)
        def _():
            pl.semaphore_wait(barrier, len(neighbours))

    cot_copies[0].wait()
    if split_first:
        first_copy(1 - core).wait()
        first_copy(core).start()
    else:
        a_copy(0, order[0]).wait()
    cot_copies[1].start()

    a_copy(1, order[1]).start()

    multiply(0, 0, meet, lambda: first_copy(core).wait())
    cot_copies[1].wait()
    multiply(0, 1, None, lambda: finish(0, 0))
    if not split_first:
        finish(0, 0)

    def body(i, carry):
        pltpu.make_async_copy(
            a_hbm.at[:, pl.ds(0, tall)], a_ref.at[i], a_sem.at[i]
        ).wait()

        for j, k in enumerate(order[2:]):
            @pl.when(i == j + 1)
            def _():
                a_copy(j + 2, k).start()

        multiply(i, 0)

        finish(i - 1, 1)

        multiply(i, 1)
        finish(i, 0)
        return carry

    lax.fori_loop(1, blocks, body, 0)
    finish(blocks - 1, 1)

    for r in range(roles):
        @pl.when(role == r)
        def _():
            perform(final[r])
            for n, shape in enumerate(shapes):
                sent = sum((m.rows, parts[m.part][4]) == shape and m.sender == r for m in messages)
                if sent:
                    every = landing[shape].at[pl.ds(0, sent)]
                    pltpu.make_async_remote_copy(
                        src_ref=every, dst_ref=every, send_sem=send_sem.at[n],
                        recv_sem=recv_sem.at[0], device_id=partner("x"), device_id_type=MESH,
                    ).wait_send()

    pltpu.make_async_remote_copy(
        src_ref=mate_ref, dst_ref=mate_ref, send_sem=mate_send,
        recv_sem=recv_sem.at[0], device_id=partner("core"), device_id_type=MESH,
    ).wait_send()


def landing_indices(parts, messages):
    counts, indices = {}, {}
    for message in messages:
        shape = message.rows, parts[message.part][4]
        if message.slot not in indices:
            indices[message.slot] = counts.get(shape, 0)
            counts[shape] = counts.get(shape, 0) + 1
    return indices


def landing_shapes(parts, messages):
    counts = {}
    for slot, message in {m.slot: m for m in messages}.items():
        shape = message.rows, parts[message.part][4]
        counts[shape] = counts.get(shape, 0) + 1
    return dict(sorted(counts.items(), reverse=True))


def cut(rows, columns):
    return tuple(
        (way, rows * top // 8, rows * tall // 8, columns * left // 8, columns * wide // 8)
        for way, top, tall, left, wide in PARTS
    )


def local(mesh_shape, activations, key_cotangent, value_cotangent):
    tokens, width = activations.shape
    half = key_cotangent.shape[1]
    rows = width // mesh_shape["intra"]
    groups = mesh_shape["intra"] // 4
    blocks = 2 * groups
    parts = cut(rows, 2 * half)
    messages = plan_messages(groups, parts)
    order = block_order(groups)
    steps = compute_steps(order, half, TUNE)
    plan = schedule(groups, parts, messages, steps, TUNE)
    names = {message.slot for message in messages}
    f32 = jnp.float32
    landing = [
        pltpu.VMEM((count, *shape), f32)
        for shape, count in landing_shapes(parts, messages).items()
    ]
    totals = pl.pallas_call(
        functools.partial(kernel, mesh_shape, parts, messages, order, plan),
        out_shape=(pltpu.VMEM((rows, half), f32),) * 2,
        in_specs=[pl.BlockSpec(memory_space=pl.ANY)] * 3,
        out_specs=(pl.BlockSpec(memory_space=pltpu.VMEM),) * 2,
        scratch_shapes=[
            pltpu.VMEM((blocks, tokens, 2 * rows), activations.dtype),
            pltpu.VMEM((tokens, 2 * half), key_cotangent.dtype),
            pltpu.VMEM((blocks, 2, rows, 2 * half), f32),
            pltpu.VMEM((blocks, 2, rows, half), f32),
            *landing,
            pltpu.SemaphoreType.DMA((blocks,)),
            pltpu.SemaphoreType.DMA((2,)),
            pltpu.SemaphoreType.DMA((2,)),
            pltpu.SemaphoreType.DMA,
            pltpu.SemaphoreType.DMA((blocks, 2)),
            pltpu.SemaphoreType.DMA((len(landing),)),
            pltpu.SemaphoreType.DMA((len(names),)),
        ],
        compiler_params=pltpu.CompilerParams(
            collective_id=0, has_side_effects=True, vmem_limit_bytes=65900000
        ),
    )(activations, key_cotangent, value_cotangent)
    shape = jax.ShapeDtypeStruct((rows, half), f32)
    return pl.pallas_call(
        write_out,
        out_shape=(shape, shape),
        in_specs=[pl.BlockSpec(memory_space=pltpu.VMEM)] * 2,
        out_specs=(pl.BlockSpec(memory_space=pltpu.HBM),) * 2,
        scratch_shapes=[pltpu.SemaphoreType.DMA((2,))],
    )(*[pltpu.with_memory_space_constraint(total, pltpu.VMEM) for total in totals])


def write_out(key_ref, value_ref, key_out, value_out, sem):
    copies = [
        pltpu.make_async_copy(key_ref, key_out, sem.at[0]),
        pltpu.make_async_copy(value_ref, value_out, sem.at[1]),
    ]
    for copy in copies:
        copy.start()
    for copy in copies:
        copy.wait()


def solution(mesh):
    mesh_shape = dict(mesh.shape)
    return jax.shard_map(
        functools.partial(local, mesh_shape),
        mesh=mesh,
        in_specs=(
            P(("inter", "intra"), None),
            P(("inter", "intra"), None),
            P(("inter", "intra"), None),
        ),
        out_specs=(P("intra", None), P("intra", None)),
        check_vma=False,
    )
```

```python
import functools
import heapq

import jax
import jax.numpy as jnp
from jax import lax
from jax.experimental import pallas as pl
from jax.experimental.pallas import tpu as pltpu
from jax.sharding import PartitionSpec as P

MESH = pl.DeviceIdType.MESH
PARTS = (
    ('zxy', 0, 2, 0, 2),
    ('xzy', 2, 6, 0, 2),
    ('yxz', 0, 8, 2, 1),
    ('yxz', 0, 8, 3, 1),
    ('xyz', 0, 8, 4, 2),
    ('zyx', 0, 4, 6, 2),
    ('yxz', 4, 4, 6, 2),
)
TUNE = {
    "first": 4.75, "strip": 2.0, "second": 8.75, "step": 1.6, "latency": 1.95, "ahead": 4.9, "rate": 46600.0, "margin": 1.3, "cost": 0.08,
    "rank": {(4, 2): 136.8, (5, 2): 148.2, (7, 1): -73.0, (3, 3): -37.4, (5, 3): 40.1, (5, 0): -54.4, (0, 2): 28.2, (2, 2): -78.9, (2, 1): -12.0, (3, 1): -12.0, (4, 0): 71.2, (2, 0): -81.1, (0, 0): 102.4, (1, 0): 11.9, (3, 0): -19.4, (7, 2): -55.8, (6, 3): 75.4, (0, 1): 110.2, (7, 3): -44.7, (6, 1): -14.5, (1, 2): 82.7, (1, 3): 150.8, (4, 1): -84.3, (0, 3): -94.7, (7, 0): 34.6, (6, 2): 136.5, (3, 2): -63.2, (5, 1): 148.4, (1, 1): -30.4, (4, 3): -64.4, (2, 3): -120.0, (6, 0): 24.6, (8, 0): -52.8, (9, 1): -43.3, (9, 2): 50.0, (9, 3): -11.1, (8, 2): -5.8, (8, 1): 109.3, (9, 0): 29.9, (8, 3): -59.2},
}


class Message:
    def __init__(self, part, stage, kind, sender, block, receiver, target, rows, split, slot):
        self.part, self.stage, self.kind = part, stage, kind
        self.sender, self.block = sender, block
        self.receiver, self.target = receiver, target
        self.rows, self.split, self.slot = rows, split, slot


def plan_messages(groups, parts):
    roles, messages = groups // 2, []
    for part, (order, _, rows, _, _) in enumerate(parts):
        split, reduced, sides = False, False, (0, 1)

        def add(stage, kind, sender, block, receiver, target, name):
            slot = (part, stage, name)
            messages.append(
                Message(part, stage, kind, sender, block, receiver, target, rows, split, slot)
            )

        for stage, axis in enumerate(order):
            last = stage == len(order) - 1
            if axis == "x":
                sides = (0,)
            elif axis == "y" and not last:
                rows, split = rows // 2, True
            for role in range(roles):
                own = [role] if reduced else range(groups)
                if axis == "x":
                    for q in own:
                        name = ("x", -1 if reduced else q)
                        add(stage, "x", role, (q, 1), role, (q, 0), name)
                elif axis == "y" and last:
                    add(stage, "both", role, (role, 0), role, (role, 0), ("both",))
                elif axis == "y":
                    for q in own:
                        for side in sides:
                            name = ("y", -1 if reduced else q, side)
                            add(stage, "y", role, (q, side), role, (q, side), name)
                else:
                    for side in sides:
                        for q in range(role + 1, groups):
                            if role + 1 < roles:
                                name, there, to = ("in", q, side), q, role + 1
                            else:
                                there, to = groups - 1 - q, role
                                name = ("across", there, side)
                            add(stage, "in", role, (q, side), to, (there, side), name)
                        for q in range(role):
                            name = ("out", q, side)
                            add(stage, "out", role, (q, side), role - 1, (q, side), name)
            reduced = reduced or axis == "z"
        if split:
            for role in range(roles):
                add(len(order), "gather", role, (role, 0), role, (role, 0), ("gather",))
    return messages


def link_of(message):
    kind = message.kind
    return message.sender, "y" if kind in ("both", "gather") else kind


def compute_steps(order, half, tune):
    steps = []
    for i, k in enumerate(order):
        for h in (0, 1):
            at = tune["second"] + tune["step"] * (2 * (i - 1) + h)
            if not i:
                at = tune["first"] + tune["strip"] * h
            steps.append((k, h * half, (h + 1) * half, at))
    return steps


def schedule(groups, parts, messages, steps, tune):
    roles, latency = groups // 2, tune["latency"]
    incoming = {}
    for message in messages:
        incoming.setdefault((message.receiver, message.part, message.target), []).append(message)

    def needed(message):
        before = incoming.get((message.sender, message.part, message.block), [])
        same = {"in": ("in",), "out": ("out", "across")}.get(message.kind, ())
        return [
            o for o in before
            if o.stage < message.stage or (o.stage == message.stage and o.slot[2][0] in same)
        ]

    need = {m: needed(m) for m in messages}
    feeds = {m: [] for m in messages}
    for m in messages:
        for o in need[m]:
            feeds[o].append(m)

    def length(message):
        return message.rows * parts[message.part][4] * 4 / tune["rate"]

    @functools.cache
    def tail(message):
        return latency + length(message) + max((tail(o) for o in feeds[message]), default=0.0)

    def priority(message):
        return tail(message) + tune["rank"].get((message.part, message.stage), 0.0)

    def step_of(part, block):
        start = parts[part][3]
        return next(n for n, (k, low, high, _) in enumerate(steps) if k == block and low <= start < high)

    made_in = {m: step_of(m.part, m.block) for m in messages}
    kept_in = {m: step_of(m.part, m.target) for m in messages}
    slots = {(role, n): [] for role in range(roles) for n in range(len(steps))}
    final = {role: [] for role in range(roles)}
    left = {m: len(need[m]) for m in messages}
    done = {role: -1 for role in range(roles)}
    clock = {role: 0.0 for role in range(roles)}
    pending = {role: len(steps) for role in range(roles)}
    waiting = {role: [] for role in range(roles)}
    queued, free = {}, {}
    events = [(step[3], n, role, n, None) for n, step in enumerate(steps) for role in range(roles)]
    heapq.heapify(events)
    number, last = len(events), len(steps) - 1

    def enqueue(message):
        queued.setdefault(link_of(message), []).append(message)

    def release(role, now):
        nonlocal number
        started = []
        for link, queue in queued.items():
            if link[0] != role or not queue:
                continue
            queue.sort(key=priority, reverse=True)
            while queue and (free.get(link, 0.0) - now < tune["ahead"] or not pending[role]):
                message = queue.pop(0)
                begin = max(now, free.get(link, 0.0))
                free[link] = begin + length(message)
                number += 1
                pending[message.receiver] += 1
                heapq.heappush(events, (free[link] + latency, number, message.receiver, None, message))
                started.append(message)
        return started

    def accept(message):
        pending[message.receiver] -= 1
        for later in feeds[message]:
            left[later] -= 1
            if not left[later] and made_in[later] <= done[later.sender]:
                enqueue(later)

    while events:
        now, _, role, n, message = heapq.heappop(events)
        if message is not None:
            if done[role] < last:
                waiting[role].append((now, message))
                continue
            now = max(now, clock[role])
            clock[role] = now + tune["cost"]
            accept(message)
            final[role].append((message, release(role, now)))
            continue
        done[role] = n
        pending[role] -= 1
        for message in messages:
            if message.sender == role and made_in[message] == n and not left[message]:
                enqueue(message)
        slots[role, n].append((None, release(role, now)))
        actions = final[role] if n == last else slots[role, n]
        for entry in list(waiting[role]):
            at, message = entry
            if (at < now - tune["margin"] or n == last) and kept_in[message] <= n:
                waiting[role].remove(entry)
                accept(message)
                actions.append((message, release(role, now)))
    assert not any(queued.values()) and not any(waiting.values())
    return slots, final


def block_order(groups):
    order = [(q, side) for q in reversed(range(groups)) for side in (1, 0)]
    if groups == 4:
        order = [(3, 1), (3, 0), (0, 0), (2, 1), (1, 1), (2, 0), (1, 0), (0, 1)]
    return order


def kernel(
    mesh_shape, parts, messages, order, plan,
    a_hbm, key_hbm, value_hbm, key_out, value_out,
    a_ref, cot_ref, pair_ref, mate_ref, *rest,
):
    shapes = landing_shapes(parts, messages)
    landing = dict(zip(shapes, rest))
    a_sem, first_sem, cot_sem, mate_send, mate_recv, send_sem, recv_sem = rest[len(shapes):]
    slots, final = plan
    groups = mesh_shape["intra"] // 4
    roles = groups // 2
    blocks = 2 * groups
    rows = key_out.shape[0]
    tall = 2 * rows
    half = key_hbm.shape[1]
    place = {k: i for i, k in enumerate(order)}
    numbers = semaphore_numbers(messages)
    indices = landing_indices(parts, messages)

    y = lax.axis_index("inter")
    me = lax.axis_index("intra")
    core = me % 2
    x = (me // 2) % 2
    group = me // 4
    far = group // roles
    role = group + far * (groups - 1 - 2 * group)
    inward = 4 * (1 - 2 * far)

    def partner(kind):
        if kind == "core":
            return {"intra": me + 1 - 2 * core}
        if kind == "x":
            return {"intra": me + 2 * (1 - 2 * x)}
        if kind == "in":
            return {"intra": me + inward}
        if kind == "out":
            return {"intra": me - inward}
        return {"inter": 1 - y}

    cot_copies = [
        pltpu.make_async_copy(key_hbm, cot_ref.at[:, pl.ds(0, half)], cot_sem.at[0]),
        pltpu.make_async_copy(value_hbm, cot_ref.at[:, pl.ds(half, half)], cot_sem.at[1]),
    ]

    def a_copy(i, k):
        q, side = k
        block = 2 * (q + far * (groups - 1 - 2 * q)) + (x + side) % 2
        columns = pl.ds(pl.multiple_of(block * tall, tall), tall)
        return pltpu.make_async_copy(a_hbm.at[:, columns], a_ref.at[i], a_sem.at[i % 2])

    tokens = a_hbm.shape[0]
    split_first = rows % 128 == 0

    def first_copy(owner, part, parts_of):
        q, side = order[0]
        block = 2 * (q + far * (groups - 1 - 2 * q)) + (x + side) % 2
        deep = pl.ds(part * tokens // parts_of, tokens // parts_of)
        columns = pl.ds(pl.multiple_of((2 * block + owner) * rows, rows), rows)
        lanes = pl.ds(pl.multiple_of(owner * rows, rows), rows)
        return pltpu.make_async_copy(
            a_hbm.at[deep, columns], a_ref.at[0, deep, lanes], first_sem.at[part + 2 * (parts_of < 2)]
        )

    def first_cot(part):
        deep = pl.ds(part * tokens // 2, tokens // 2)
        return pltpu.make_async_copy(
            key_hbm.at[deep], cot_ref.at[deep, pl.ds(0, half)], first_sem.at[3 + part]
        )

    if split_first:
        for part in range(2):
            first_copy(1 - core, part, 2).start()
            first_cot(part).start()
    else:
        cot_copies[0].start()
        a_copy(0, order[0]).start()

    barrier = pltpu.get_barrier_semaphore()
    neighbours = ["core", "x", "y", "in"]
    for kind in neighbours:
        pl.semaphore_signal(barrier, inc=1, device_id=partner(kind), device_id_type=MESH)

    @pl.when(role > 0)
    def _():
        pl.semaphore_signal(barrier, inc=1, device_id=partner("out"), device_id_type=MESH)

    def side_of(h):
        return pl.ds(h * half, half)

    def mate_copy(i, h):
        return pltpu.make_async_remote_copy(
            src_ref=pair_ref.at[i, 1 - core, :, side_of(h)],
            dst_ref=mate_ref.at[i % 2, h],
            send_sem=mate_send,
            recv_sem=mate_recv.at[i % 2, h],
            device_id=partner("core"),
            device_id_type=MESH,
        )

    def rows_of(message, mine):
        base = parts[message.part][1]
        if not message.split:
            return pl.ds(base, message.rows)
        half_of = y if mine else 1 - y
        return pl.ds(pl.multiple_of(base + half_of * message.rows, 8), message.rows)

    def columns_of(message):
        return pl.ds(parts[message.part][3], parts[message.part][4])

    def result(message, mine):
        base, width = parts[message.part][3:]
        out, start = (key_out, base) if base < half else (value_out, base - half)
        return out.at[rows_of(message, mine), pl.ds(start, width)]

    def kept(message, block):
        return pair_ref.at[place[block], core, rows_of(message, True), columns_of(message)]

    def arrived(message):
        shape = message.rows, parts[message.part][4]
        return landing[shape].at[indices[message.slot]]

    def remote(message):
        number = numbers[message.slot]
        mine = message.kind != "y"
        return pltpu.make_async_remote_copy(
            src_ref=pair_ref.at[
                place[message.block], core, rows_of(message, mine), columns_of(message)
            ],
            dst_ref=arrived(message),
            send_sem=send_sem.at[list(shapes).index((message.rows, parts[message.part][4]))],
            recv_sem=recv_sem.at[number],
            device_id=partner(message.kind),
            device_id_type=MESH,
        )

    def perform(actions):
        for message, follow in actions:
            if message is not None:
                remote(message).wait_recv()
                if message.kind == "both":
                    total = kept(message, message.target)[...] + arrived(message)[...]
                    result(message, True)[...] = total
                elif message.kind == "gather":
                    result(message, False)[...] = arrived(message)[...]
                else:
                    kept(message, message.target)[...] += arrived(message)[...]
            for later in follow:
                remote(later).start()
                if later.kind == "gather":
                    result(later, True)[...] = kept(later, later.block)[...]

    def run(role_steps):
        for r in range(roles):
            for chosen, n in role_steps:
                if any(message or follow for message, follow in slots[r, n]):
                    @pl.when(chosen & (role == r))
                    def _():
                        perform(slots[r, n])

    def product(i, h, lanes):
        exact = lax.dot_general(
            a_ref[i, :, lanes], cot_ref[:, side_of(h)], (((0,), (0,)), ((), ())),
            preferred_element_type=jnp.float32,
        )
        return exact.astype(jnp.bfloat16).astype(jnp.float32)

    def multiply_one(i, h, owner):
        lanes = pl.ds(pl.multiple_of(owner * rows, rows), rows)
        pair_ref[i, owner, :, side_of(h)] = product(i, h, lanes)

    def multiply(i, h, enter=None, between=None):
        whole = not (split_first and isinstance(i, int))
        if whole:
            pair_ref[i, :, :, side_of(h)] = product(i, h, pl.ds(0, tall)).reshape(2, rows, half)
        else:
            multiply_one(i, h, 1 - core)
        if enter:
            enter()
        mate_copy(i, h).start()
        if between and not whole:
            between()
        if not whole:
            multiply_one(i, h, core)

    def finish(i, h):
        mate_copy(i, h).wait_recv()
        pair_ref[i, core, :, side_of(h)] += mate_ref[i % 2, h]
        if isinstance(i, int):
            run([(role >= 0, 2 * i + h)])
        else:
            run([(i == j, 2 * j + h) for j in range(1 - h, blocks - h)])

    def meet():
        @pl.when(role > 0)
        def _():
            pl.semaphore_wait(barrier, len(neighbours) + 1)

        @pl.when(role == 0)
        def _():
            pl.semaphore_wait(barrier, len(neighbours))

    if split_first:
        lanes = pl.ds(pl.multiple_of((1 - core) * rows, rows), rows)
        total = None
        for part in range(2):
            deep = pl.ds(part * tokens // 2, tokens // 2)
            first_copy(1 - core, part, 2).wait()
            first_cot(part).wait()
            if part:
                first_copy(core, 0, 1).start()
                cot_copies[1].start()
                a_copy(1, order[1]).start()
            exact = lax.dot_general(
                a_ref[0, deep, lanes], cot_ref[deep, pl.ds(0, half)], (((0,), (0,)), ((), ())),
                preferred_element_type=jnp.float32,
            )
            total = total + exact if part else exact
        pair_ref[0, 1 - core, :, side_of(0)] = total.astype(jnp.bfloat16).astype(jnp.float32)
        meet()
        mate_copy(0, 0).start()
        first_copy(core, 0, 1).wait()
        multiply_one(0, 0, core)
    else:
        cot_copies[0].wait()
        a_copy(0, order[0]).wait()
        cot_copies[1].start()
        a_copy(1, order[1]).start()
        multiply(0, 0, meet)
    cot_copies[1].wait()
    multiply(0, 1, None, lambda: finish(0, 0))
    if not split_first:
        finish(0, 0)

    def body(i, carry):
        pltpu.make_async_copy(
            a_hbm.at[:, pl.ds(0, tall)], a_ref.at[i], a_sem.at[i % 2]
        ).wait()

        for j, k in enumerate(order[2:]):
            @pl.when(i == j + 1)
            def _():
                a_copy(j + 2, k).start()

        multiply(i, 0)

        finish(i - 1, 1)

        multiply(i, 1)
        finish(i, 0)
        return carry

    lax.fori_loop(1, blocks, body, 0)
    finish(blocks - 1, 1)

    for r in range(roles):
        @pl.when(role == r)
        def _():
            perform(final[r])
            for n, shape in enumerate(shapes):
                sent = sum((m.rows, parts[m.part][4]) == shape and m.sender == r for m in messages)
                if sent:
                    every = landing[shape].at[pl.ds(0, sent)]
                    pltpu.make_async_remote_copy(
                        src_ref=every, dst_ref=every, send_sem=send_sem.at[n],
                        recv_sem=recv_sem.at[0], device_id=partner("x"), device_id_type=MESH,
                    ).wait_send()

    every = pair_ref.at[:, 0]
    pltpu.make_async_remote_copy(
        src_ref=every, dst_ref=every, send_sem=mate_send,
        recv_sem=recv_sem.at[0], device_id=partner("core"), device_id_type=MESH,
    ).wait_send()


def semaphore_numbers(messages):
    receivers, taken, numbers = {}, [], {}
    for message in messages:
        receivers.setdefault(message.slot, set()).add(message.receiver)
    for slot, roles in receivers.items():
        free = [n for n, others in enumerate(taken) if not others & roles]
        if not free:
            free = [len(taken)]
            taken.append(set())
        numbers[slot] = free[0]
        taken[free[0]] |= roles
    return numbers


def landing_indices(parts, messages):
    counts, indices = {}, {}
    for message in messages:
        shape = message.rows, parts[message.part][4]
        if message.slot not in indices:
            indices[message.slot] = counts.get(shape, 0)
            counts[shape] = counts.get(shape, 0) + 1
    return indices


def landing_shapes(parts, messages):
    counts = {}
    for slot, message in {m.slot: m for m in messages}.items():
        shape = message.rows, parts[message.part][4]
        counts[shape] = counts.get(shape, 0) + 1
    return dict(sorted(counts.items(), reverse=True))


def cut(rows, columns):
    return tuple(
        (way, rows * top // 8, rows * tall // 8, columns * left // 8, columns * wide // 8)
        for way, top, tall, left, wide in PARTS
    )


def local(mesh_shape, activations, key_cotangent, value_cotangent):
    tokens, width = activations.shape
    half = key_cotangent.shape[1]
    rows = width // mesh_shape["intra"]
    groups = mesh_shape["intra"] // 4
    blocks = 2 * groups
    parts = cut(rows, 2 * half)
    messages = plan_messages(groups, parts)
    order = block_order(groups)
    steps = compute_steps(order, half, TUNE)
    plan = schedule(groups, parts, messages, steps, TUNE)
    received = max(semaphore_numbers(messages).values()) + 1
    f32 = jnp.float32
    landing = [
        pltpu.VMEM((count, *shape), f32)
        for shape, count in landing_shapes(parts, messages).items()
    ]
    totals = pl.pallas_call(
        functools.partial(kernel, mesh_shape, parts, messages, order, plan),
        out_shape=(pltpu.VMEM((rows, half), f32),) * 2,
        in_specs=[pl.BlockSpec(memory_space=pl.ANY)] * 3,
        out_specs=(pl.BlockSpec(memory_space=pltpu.VMEM),) * 2,
        scratch_shapes=[
            pltpu.VMEM((blocks, tokens, 2 * rows), activations.dtype),
            pltpu.VMEM((tokens, 2 * half), key_cotangent.dtype),
            pltpu.VMEM((blocks, 2, rows, 2 * half), f32),
            pltpu.VMEM((2, 2, rows, half), f32),
            *landing,
            pltpu.SemaphoreType.DMA((2,)),
            pltpu.SemaphoreType.DMA((5,)),
            pltpu.SemaphoreType.DMA((2,)),
            pltpu.SemaphoreType.DMA,
            pltpu.SemaphoreType.DMA((2, 2)),
            pltpu.SemaphoreType.DMA((len(landing),)),
            pltpu.SemaphoreType.DMA((received,)),
        ],
        compiler_params=pltpu.CompilerParams(
            collective_id=0, has_side_effects=True, vmem_limit_bytes=65900000
        ),
    )(activations, key_cotangent, value_cotangent)
    shape = jax.ShapeDtypeStruct((rows, half), f32)
    return pl.pallas_call(
        write_out,
        out_shape=(shape, shape),
        in_specs=[pl.BlockSpec(memory_space=pltpu.VMEM)] * 2,
        out_specs=(pl.BlockSpec(memory_space=pltpu.HBM),) * 2,
        scratch_shapes=[pltpu.SemaphoreType.DMA((2,))],
    )(*[pltpu.with_memory_space_constraint(total, pltpu.VMEM) for total in totals])


def write_out(key_ref, value_ref, key_out, value_out, sem):
    copies = [
        pltpu.make_async_copy(key_ref, key_out, sem.at[0]),
        pltpu.make_async_copy(value_ref, value_out, sem.at[1]),
    ]
    for copy in copies:
        copy.start()
    for copy in copies:
        copy.wait()


def solution(mesh):
    mesh_shape = dict(mesh.shape)
    return jax.shard_map(
        functools.partial(local, mesh_shape),
        mesh=mesh,
        in_specs=(
            P(("inter", "intra"), None),
            P(("inter", "intra"), None),
            P(("inter", "intra"), None),
        ),
        out_specs=(P("intra", None), P("intra", None)),
        check_vma=False,
    )
```
